32 devices in a mesh: dp: 4 (over y, x), mp: 8 (over z, core).
Axes of the slice: x: 2, y: 2, z: 4, core: 2. Of those that a mesh axis runs over, the one named last changes fastest.
Arguments:
- tokens: bfloat16 [128, 6144], P(('dp', 'mp')), may hold values from -6 to 6
- norm_gain: float32 [6144], replicated, may hold values from 0.5 to 1.5
- w_query: bfloat16 [6144, 4096], P('dp', 'mp'), as said below
- w_key: bfloat16 [6144, 4096], P('dp', 'mp'), as said below
- w_value: bfloat16 [6144, 4096], P('dp', 'mp'), may hold values from -0.078125 to 0.078125
- w_inner: bfloat16 [6144, 24576], P('dp', 'mp'), may hold values from -0.078125 to 0.078125
- bias_inner: float32 [24576], P('mp'), may hold values from -3 to 3
- w_attn_out: bfloat16 [4096, 6144], P('mp', 'dp'), may hold values from -0.09375 to 0.09375
- w_outer: bfloat16 [24576, 6144], P('mp', 'dp'), may hold values from -0.0390625 to 0.0390625
- temper: float32 [32], P('mp'), may hold values from 0.5 to 24
Outputs:
- result: bfloat16 [128, 6144], P(('dp', 'mp'))
The draws below stay inside these ranges and needn't reach their ends.
Inputs may be any that keep to these rules, and one draw needn't show every extreme that they name: `w_query`: entries of order 6144 ** -0.5. `w_key`: entries of order 6144 ** -0.5.
All inputs are finite; a program needn't handle non-finite values.
Results may differ from the reference program's by a relative error of at most 0.023.
Values may be sent and summed in bfloat16 or wider, within the bound.
A program may use at most 128 MiB of HBM per device.

```python
import math
import jax
import jax.numpy as jnp
from jax import lax

D = 6144
HEADS = 32
HEAD = 128
FF = 24576
HD = 4096
PATCHES = 32
TOKENS = 128
N_DP = 4


def shared_draws(key):
    key_query = jax.random.fold_in(key, 11)
    key_noise = jax.random.fold_in(key, 12)
    key_temper = jax.random.fold_in(key, 14)
    scale = D ** (-0.5)
    limit = 6.0 * scale
    query = jnp.clip(jax.random.normal(key_query, (D, HD), jnp.float32) * scale, -limit, limit)
    noise = jnp.clip(jax.random.normal(key_noise, (D, HD), jnp.float32) * scale, -limit, limit)
    temper = jnp.exp(jax.random.uniform(key_temper, (HEADS,), jnp.float32, jnp.log(0.5), jnp.log(6.0)))
    keys = noise
    return (query, keys, temper)


def draw_w_query(key, part):
    return shared_draws(key)[0].astype(jnp.bfloat16)


def draw_w_key(key, part):
    return shared_draws(key)[1].astype(jnp.bfloat16)


def draw_temper(key, part):
    return shared_draws(key)[2]


def level_of(rng, extent, split, low, high):
    level, own = 1.0, jax.random.fold_in(rng, 6)
    for dim, blocks in split:
        heights = jnp.exp(jax.random.uniform(jax.random.fold_in(own, dim), (blocks,), jnp.float32, low / len(split), high / len(split)))
        level = level * jnp.repeat(heights, extent[dim] // blocks).reshape([-1 if axis == dim else 1 for axis in range(len(extent))])
    return level


def bell_draw(stream_key, extent, deviation, most, shards=(), kind=jnp.bfloat16):
    result = deviation * jax.random.normal(stream_key, extent, jnp.float32)
    if shards:
        result = result * level_of(stream_key, extent, shards, -0.22, 0.18)
    return jnp.clip(result, -most, most).astype(kind)


def setup_inputs(seed: int = 0) -> dict:
    streams_of = jax.random.split(jax.random.key(seed), 11)
    return {
        "tokens": bell_draw(streams_of[0], (TOKENS, D), 1.0, 6.0, ((0, 32),)),
        "norm_gain": jnp.clip(1.0 + 0.1 * jax.random.normal(streams_of[1], (D,), jnp.float32), 0.5, 1.5),
        "w_query": draw_w_query(jax.random.fold_in(streams_of[10], 71), 0),
        "w_key": draw_w_key(jax.random.fold_in(streams_of[10], 71), 0),
        "w_value": bell_draw(streams_of[4], (D, HD), D ** -0.5, 0.078125, ((0, 4), (1, 8))),
        "w_inner": bell_draw(streams_of[5], (D, FF), D ** -0.5, 0.078125, ((0, 4), (1, 8))),
        "bias_inner": bell_draw(streams_of[6], (FF,), 0.5, 3.0, ((0, 8),), jnp.float32),
        "w_attn_out": bell_draw(streams_of[7], (HD, D), HD ** -0.5, 0.09375, ((0, 8), (1, 4))),
        "w_outer": bell_draw(streams_of[8], (FF, D), FF ** -0.5, 0.0390625, ((0, 8), (1, 4))),
        "temper": draw_temper(jax.random.fold_in(streams_of[10], 71), 0),
    }


def normalize(values):
    center = values - lax.optimization_barrier(jnp.mean(values, axis=-1, keepdims=True))
    spread = lax.optimization_barrier(jnp.mean(center * center, axis=-1, keepdims=True))
    return center * lax.rsqrt(spread + 1e-06)

def reference(tokens, norm_gain, w_query, w_key, w_value, w_inner, bias_inner, w_attn_out, w_outer, temper):
    local = tokens.astype(jnp.float32)
    normed = (normalize(local) * norm_gain.astype(jnp.float32)).astype(jnp.bfloat16)
    query = jnp.dot(normed, w_query, preferred_element_type=jnp.float32).astype(jnp.bfloat16)
    keys = jnp.dot(normed, w_key, preferred_element_type=jnp.float32).astype(jnp.bfloat16)
    values = jnp.dot(normed, w_value, preferred_element_type=jnp.float32).astype(jnp.bfloat16)
    shape = (N_DP, PATCHES, HEADS, HEAD)
    query_norm = normalize(query.astype(jnp.float32).reshape(shape)).astype(jnp.bfloat16)
    key_norm = normalize(keys.astype(jnp.float32).reshape(shape)).astype(jnp.bfloat16)
    values4 = values.reshape(shape).astype(jnp.float32)
    scale = temper.astype(jnp.float32) / math.sqrt(HEAD)
    scores = jnp.einsum('bqhc,bkhc->bhqk', query_norm.astype(jnp.float32), key_norm.astype(jnp.float32))
    scores = scores * scale[None, :, None, None]
    probs = jax.nn.softmax(scores, axis=-1).astype(jnp.bfloat16)
    mixed = jnp.einsum('bhqk,bkhc->bqhc', probs.astype(jnp.float32), values4)
    mixed = mixed.astype(jnp.bfloat16).reshape(TOKENS, HD)
    inner = jnp.dot(normed, w_inner, preferred_element_type=jnp.float32) + bias_inner.astype(jnp.float32)
    activ = jax.nn.gelu(inner, approximate=False).astype(jnp.bfloat16)
    total = jnp.dot(mixed, w_attn_out, preferred_element_type=jnp.float32)
    total = total + jnp.dot(activ, w_outer, preferred_element_type=jnp.float32)
    return (local + total).astype(jnp.bfloat16)
```

```python
import math

import jax
import jax.numpy as jnp
from jax import lax
from jax.sharding import PartitionSpec as P

HEAD = 128


def normalize(values):
    center = values - jnp.mean(values, axis=-1, keepdims=True)
    spread = jnp.mean(center * center, axis=-1, keepdims=True)
    return center * lax.rsqrt(spread + 1e-06)


def per_device(
    tokens, norm_gain, w_query, w_key, w_value, w_inner, bias_inner, w_attn_out, w_outer, temper
):
    f32, bf16 = jnp.float32, jnp.bfloat16
    n_dp, n_mp = lax.axis_size("dp"), lax.axis_size("mp")
    local = tokens.astype(f32)
    rows = tokens.shape[0]
    normed = (normalize(local) * norm_gain).astype(bf16)
    part = lax.all_to_all(normed.reshape(rows, n_dp, -1), "dp", split_axis=1, concat_axis=0)
    part = part.reshape(n_dp, rows, -1)
    spread = lax.all_gather(part, "mp", axis=1)
    spread = spread.reshape(n_dp * n_mp * rows, -1)

    def project(weight):
        out = jnp.dot(spread, weight, preferred_element_type=f32).astype(bf16)
        return out

    width_head = w_query.shape[1]
    stacked = jnp.concatenate([project(w) for w in (w_query, w_key, w_value, w_inner)], axis=1)
    projected = lax.psum_scatter(stacked, "dp", scatter_dimension=0, tiled=True).astype(f32)
    count_rows = n_mp * rows
    heads_dev = width_head // HEAD
    shape = (count_rows, heads_dev, HEAD)
    query_norm = normalize(projected[:, :width_head].reshape(shape)).astype(bf16)
    key_norm = normalize(projected[:, width_head : 2 * width_head].reshape(shape)).astype(bf16)
    values = projected[:, 2 * width_head : 3 * width_head].astype(bf16).reshape(shape)
    scale = temper / math.sqrt(HEAD)
    scores = jnp.einsum("qhc,khc->hqk", query_norm, key_norm, preferred_element_type=f32)
    scores = scores * scale[:, None, None]
    probs = jax.nn.softmax(scores, axis=-1).astype(bf16)
    mixed = jnp.einsum("hqk,khc->qhc", probs, values, preferred_element_type=f32)
    mixed = mixed.astype(bf16).reshape(count_rows, width_head)
    inner = projected[:, 3 * width_head :] + bias_inner
    activ = jax.nn.gelu(inner, approximate=False).astype(bf16)
    hidden = lax.all_gather(jnp.concatenate((mixed, activ), axis=1), "dp", axis=0, tiled=True)
    out = jnp.dot(hidden[:, :width_head], w_attn_out, preferred_element_type=f32)
    out = out + jnp.dot(hidden[:, width_head:], w_outer, preferred_element_type=f32)
    out = out.astype(bf16).reshape(n_dp, n_mp, rows, -1)
    out = lax.psum_scatter(out, "mp", scatter_dimension=1, tiled=False)
    out = lax.all_to_all(out, "dp", split_axis=0, concat_axis=1).reshape(rows, -1)
    return (local + out.astype(f32)).astype(bf16)


def solution(mesh):
    return jax.shard_map(
        per_device,
        mesh=mesh,
        in_specs=(
            P(("dp", "mp"), None),
            P(),
            P("dp", "mp"),
            P("dp", "mp"),
            P("dp", "mp"),
            P("dp", "mp"),
            P("mp"),
            P("mp", "dp"),
            P("mp", "dp"),
            P("mp"),
        ),
        out_specs=P(("dp", "mp"), None),
        check_vma=False,
    )
```

```python
import functools
import math

import jax
import jax.numpy as jnp
from jax import lax
from jax.experimental import pallas as pl
from jax.experimental.pallas import tpu as pltpu
from jax.sharding import PartitionSpec as P

HEAD = 128
MESH = pl.DeviceIdType.MESH
F32, BF16 = jnp.float32, jnp.bfloat16


def normalize(values):
    center = values - jnp.mean(values, axis=-1, keepdims=True)
    spread = jnp.mean(center * center, axis=-1, keepdims=True)
    return center * lax.rsqrt(spread + 1e-06)


def wait_bytes(ref, sem):
    pltpu.make_async_copy(ref, ref, sem).wait()


def block_kernel(
    n_dp, n_mp,
    tokens, gain, bias, temper, w_query, w_key, w_value, w_inner, w_attn, w_outer,
    out,
    w_in, w_out, nsend, nrecv, stage, x, psend, precv, ag, acc, dsend, drecv,
    win_sem, wout_sem, a_send, a_recv, p_send, p_recv, g_send, g_recv, d_send, d_recv,
):
    n_dev = n_dp * n_mp
    rows = tokens.shape[0]
    n_in, depth, wide = w_in.shape
    n_out = w_out.shape[0]
    per = psend.shape[2]
    i, j = lax.axis_index("dp"), lax.axis_index("mp")
    me = i * n_mp + j

    barrier = pltpu.get_barrier_semaphore()

    def greet(d, carry):
        t = lax.rem(me + d, n_dev)
        pl.semaphore_signal(
            barrier, inc=1, device_id=(t // n_mp, lax.rem(t, n_mp)), device_id_type=MESH
        )
        return carry

    lax.fori_loop(1, n_dev, greet, 0)

    for c, w in enumerate((w_query, w_key, w_value)):
        pltpu.make_async_copy(w, w_in.at[c], win_sem.at[c]).start()
    for c in range(3, n_in):
        pltpu.make_async_copy(
            w_inner.at[:, pl.ds((c - 3) * wide, wide)], w_in.at[c], win_sem.at[c]
        ).start()
    pltpu.make_async_copy(w_attn, w_out.at[0], wout_sem.at[0]).start()
    for c in range(1, n_out):
        pltpu.make_async_copy(
            w_outer.at[pl.ds((c - 1) * wide, wide), :], w_out.at[c], wout_sem.at[c]
        ).start()

    normed = (normalize(tokens[...].astype(F32)) * gain[...]).astype(BF16)
    for p in range(n_dp):
        nsend[p] = normed[:, p * depth : (p + 1) * depth]
    nrecv[me] = nsend[i]
    pl.semaphore_wait(barrier, n_dev - 1)

    def scatter_normed(d, carry):
        t = lax.rem(me + d, n_dev)
        ti, tj = t // n_mp, lax.rem(t, n_mp)
        pltpu.make_async_remote_copy(
            src_ref=nsend.at[ti], dst_ref=nrecv.at[me], send_sem=a_send, recv_sem=a_recv,
            device_id=(ti, tj), device_id_type=MESH,
        ).start()
        return carry

    lax.fori_loop(1, n_dev, scatter_normed, 0)
    wait_bytes(nrecv.at[pl.ds(0, n_dev - 1)], a_recv)
    for s in range(n_dev):
        stage[s * rows : (s + 1) * rows, :] = nrecv[s].astype(F32)
    x[...] = stage[...].astype(BF16)

    def project(c, carry):
        pltpu.make_async_copy(w_query, w_in.at[c], win_sem.at[c]).wait()
        part = jnp.dot(x[...], w_in[c], preferred_element_type=F32).astype(BF16)
        psend[c] = part.reshape(n_dp, per, wide)
        precv[c, i] = psend[c, i]
        for d in range(1, n_dp):
            p = lax.rem(i + d, n_dp)
            pltpu.make_async_remote_copy(
                src_ref=psend.at[c, p], dst_ref=precv.at[c, i],
                send_sem=p_send, recv_sem=p_recv.at[c],
                device_id=(p, j), device_id_type=MESH,
            ).start()
        return carry

    lax.fori_loop(0, n_in, project, 0)

    def reduced(c):
        wait_bytes(precv.at[c, pl.ds(0, n_dp - 1)], p_recv.at[c])
        total = precv[c, 0].astype(F32)
        for p in range(1, n_dp):
            total = total + precv[c, p].astype(F32)
        return total

    def share(h, value):
        ag[h, i] = value
        for d in range(1, n_dp):
            p = lax.rem(i + d, n_dp)
            pltpu.make_async_remote_copy(
                src_ref=ag.at[h, i], dst_ref=ag.at[h, i],
                send_sem=g_send, recv_sem=g_recv.at[h],
                device_id=(p, j), device_id_type=MESH,
            ).start()

    query, key, value = reduced(0), reduced(1), reduced(2)
    mixed = []
    for h in range(wide // HEAD):
        cols = slice(h * HEAD, (h + 1) * HEAD)
        query_norm = normalize(query[:, cols].astype(BF16).astype(F32)).astype(BF16)
        key_norm = normalize(key[:, cols].astype(BF16).astype(F32)).astype(BF16)
        scores = lax.dot_general(
            query_norm, key_norm, (((1,), (1,)), ((), ())), preferred_element_type=F32
        )
        scores = scores * (temper[h] * (1.0 / math.sqrt(HEAD)))
        weight = jnp.exp(scores - jnp.max(scores, axis=-1, keepdims=True))
        probs = (weight / jnp.sum(weight, axis=-1, keepdims=True)).astype(BF16)
        mixed.append(
            jnp.dot(probs, value[:, cols].astype(BF16), preferred_element_type=F32).astype(BF16)
        )
    share(0, jnp.concatenate(mixed, axis=1))

    def activate(h, carry):
        at = pl.multiple_of((h - 1) * wide, HEAD)
        inner = reduced(h + 2) + bias[:, pl.ds(at, wide)]
        activ = 0.5 * inner * (1.0 + lax.erf(inner * math.sqrt(0.5)))
        share(h, activ.astype(BF16))
        return carry

    lax.fori_loop(1, n_out, activate, 0)

    acc[...] = jnp.zeros_like(acc)

    def project_out(h, carry):
        pltpu.make_async_copy(w_attn, w_out.at[h], wout_sem.at[h]).wait()
        wait_bytes(ag.at[h, pl.ds(0, n_dp - 1)], g_recv.at[h])
        acc[...] += jnp.dot(
            ag[h].reshape(n_dp * per, wide), w_out[h], preferred_element_type=F32
        )
        return carry

    lax.fori_loop(0, n_out, project_out, 0)

    for t in range(n_dev):
        dsend[t] = acc[t * rows : (t + 1) * rows, :].astype(BF16)
    drecv[me] = dsend[me]

    def scatter_out(d, carry):
        t = lax.rem(me + d, n_dev)
        pltpu.make_async_remote_copy(
            src_ref=dsend.at[t], dst_ref=drecv.at[me], send_sem=d_send, recv_sem=d_recv,
            device_id=(t // n_mp, lax.rem(t, n_mp)), device_id_type=MESH,
        ).start()
        return carry

    lax.fori_loop(1, n_dev, scatter_out, 0)
    wait_bytes(drecv.at[pl.ds(0, n_dev - 1)], d_recv)
    for p in range(n_dp):
        total = drecv[p * n_mp].astype(F32)
        for q in range(1, n_mp):
            total = total + drecv[p * n_mp + q].astype(F32)
        cols = slice(p * depth, (p + 1) * depth)
        out[:, cols] = (tokens[:, cols].astype(F32) + total).astype(BF16)

    wait_bytes(nrecv.at[pl.ds(0, n_dev - 1)], a_send)
    wait_bytes(precv.at[:, pl.ds(0, n_dp - 1)], p_send)
    wait_bytes(ag.at[:, pl.ds(0, n_dp - 1)], g_send)
    wait_bytes(drecv.at[pl.ds(0, n_dev - 1)], d_send)


def per_device(
    n_dp, n_mp,
    tokens, norm_gain, w_query, w_key, w_value, w_inner, bias_inner, w_attn_out, w_outer, temper
):
    rows, width = tokens.shape
    depth, wide = w_query.shape
    hidden = w_inner.shape[1]
    n_dev, per = n_dp * n_mp, n_mp * rows
    n_in, n_out = 3 + hidden // wide, 1 + hidden // wide
    vmem = pl.BlockSpec(memory_space=pltpu.VMEM)
    smem = pl.BlockSpec(memory_space=pltpu.SMEM)
    hbm = pl.BlockSpec(memory_space=pl.ANY)
    dma = pltpu.SemaphoreType.DMA
    return pl.pallas_call(
        functools.partial(block_kernel, n_dp, n_mp),
        out_shape=jax.ShapeDtypeStruct((rows, width), BF16),
        in_specs=[vmem, vmem, vmem, smem] + [hbm] * 6,
        out_specs=vmem,
        scratch_shapes=[
            pltpu.VMEM((n_in, depth, wide), BF16),
            pltpu.VMEM((n_out, wide, depth), BF16),
            pltpu.VMEM((n_dp, rows, depth), BF16),
            pltpu.VMEM((n_dev, rows, depth), BF16),
            pltpu.VMEM((n_dev * rows, depth), F32),
            pltpu.VMEM((n_dev * rows, depth), BF16),
            pltpu.VMEM((n_in, n_dp, per, wide), BF16),
            pltpu.VMEM((n_in, n_dp, per, wide), BF16),
            pltpu.VMEM((n_out, n_dp, per, wide), BF16),
            pltpu.VMEM((n_dev * rows, depth), F32),
            pltpu.VMEM((n_dev, rows, depth), BF16),
            pltpu.VMEM((n_dev, rows, depth), BF16),
            dma((n_in,)), dma((n_out,)), dma, dma, dma, dma((n_in,)), dma, dma((n_out,)), dma, dma,
        ],
        compiler_params=pltpu.CompilerParams(
            collective_id=0, has_side_effects=True, vmem_limit_bytes=60 * 1024 * 1024
        ),
        name="encoder_block",
    )(
        tokens, norm_gain.reshape(1, -1), bias_inner.reshape(1, -1), temper,
        w_query, w_key, w_value, w_inner, w_attn_out, w_outer,
    )


def solution(mesh):
    return jax.shard_map(
        functools.partial(per_device, mesh.shape["dp"], mesh.shape["mp"]),
        mesh=mesh,
        in_specs=(
            P(("dp", "mp"), None),
            P(),
            P("dp", "mp"),
            P("dp", "mp"),
            P("dp", "mp"),
            P("dp", "mp"),
            P("mp"),
            P("mp", "dp"),
            P("mp", "dp"),
            P("mp"),
        ),
        out_specs=P(("dp", "mp"), None),
        check_vma=False,
    )
```

```python
import functools
import math

import jax
import jax.numpy as jnp
from jax import lax
from jax.experimental import pallas as pl
from jax.experimental.pallas import tpu as pltpu
from jax.sharding import PartitionSpec as P

HEAD = 128
MESH = pl.DeviceIdType.MESH
F32, BF16 = jnp.float32, jnp.bfloat16


def normalize(values):
    center = values - jnp.mean(values, axis=-1, keepdims=True)
    spread = jnp.mean(center * center, axis=-1, keepdims=True)
    return center * lax.rsqrt(spread + 1e-06)


def wait_bytes(ref, sem):
    pltpu.make_async_copy(ref, ref, sem).wait()


def block_kernel(
    n_dp, n_mp,
    tokens, gain, bias, temper, w_query, w_key, w_value, w_inner, w_attn, w_outer,
    out,
    w_in, w_out, nsend, nrecv, stage, x, psend, precv, ag, acc, xsend, xrecv, dsend, drecv,
    win_sem, wout_sem, a_send, a_recv, f_send, f_recv, p_send, p_recv, g_send, g_recv,
    x_send, x_recv, d_send, d_recv,
):
    n_dev = n_dp * n_mp
    rows = tokens.shape[0]
    n_in, depth, wide = w_in.shape
    n_out = w_out.shape[0]
    per = psend.shape[2]
    i, j = lax.axis_index("dp"), lax.axis_index("mp")
    me = i * n_mp + j
    n_chip = n_mp // 2
    n_lane = n_dp * n_chip
    core, chip = lax.rem(j, 2), j // 2
    sibling = (i, j + 1 - 2 * core)
    lane = i * n_chip + chip

    def same_core(other):
        return (other // n_chip, 2 * lax.rem(other, n_chip) + core)

    barrier = pltpu.get_barrier_semaphore()

    def greet(d, carry):
        t = lax.rem(me + d, n_dev)
        pl.semaphore_signal(
            barrier, inc=1, device_id=(t // n_mp, lax.rem(t, n_mp)), device_id_type=MESH
        )
        return carry

    lax.fori_loop(1, n_dev, greet, 0)

    for c, w in enumerate((w_query, w_key, w_value)):
        pltpu.make_async_copy(w, w_in.at[c], win_sem.at[c]).start()
    for c in range(3, n_in):
        pltpu.make_async_copy(
            w_inner.at[:, pl.ds((c - 3) * wide, wide)], w_in.at[c], win_sem.at[c]
        ).start()
    pltpu.make_async_copy(w_attn, w_out.at[0], wout_sem.at[0]).start()
    for c in range(1, n_out):
        pltpu.make_async_copy(
            w_outer.at[pl.ds((c - 1) * wide, wide), :], w_out.at[c], wout_sem.at[c]
        ).start()

    normed = (normalize(tokens[...].astype(F32)) * gain[...]).astype(BF16)
    for p in range(n_dp):
        nsend[p] = normed[:, p * depth : (p + 1) * depth]
    nrecv[me] = nsend[i]
    pl.semaphore_wait(barrier, n_dev - 1)

    def scatter_normed(d, carry):
        target = same_core(lax.rem(lane + d, n_lane))
        pltpu.make_async_remote_copy(
            src_ref=nsend.at[target[0]], dst_ref=nrecv.at[me],
            send_sem=a_send, recv_sem=a_recv.at[d],
            device_id=target, device_id_type=MESH,
        ).start()
        return carry

    def pass_on(source):
        pltpu.make_async_remote_copy(
            src_ref=nrecv.at[source], dst_ref=nrecv.at[source], send_sem=f_send, recv_sem=f_recv,
            device_id=sibling, device_id_type=MESH,
        ).start()

    lax.fori_loop(1, n_lane, scatter_normed, 0)
    pass_on(me)

    def forward_normed(d, carry):
        wait_bytes(nrecv.at[0], a_recv.at[d])
        source = same_core(lax.rem(lane + n_lane - d, n_lane))
        pass_on(source[0] * n_mp + source[1])
        return carry

    lax.fori_loop(1, n_lane, forward_normed, 0)
    wait_bytes(nrecv.at[pl.ds(0, n_lane)], f_recv)
    for s in range(n_dev):
        stage[s * rows : (s + 1) * rows, :] = nrecv[s].astype(F32)
    x[...] = stage[...].astype(BF16)

    def project(c, carry):
        pltpu.make_async_copy(w_query, w_in.at[c], win_sem.at[c]).wait()
        part = jnp.dot(x[...], w_in[c], preferred_element_type=F32).astype(BF16)
        psend[c] = part.reshape(n_dp, per, wide)
        precv[c, i] = psend[c, i]
        for d in range(1, n_dp):
            p = lax.rem(i + d, n_dp)
            pltpu.make_async_remote_copy(
                src_ref=psend.at[c, p], dst_ref=precv.at[c, i],
                send_sem=p_send, recv_sem=p_recv.at[c],
                device_id=(p, j), device_id_type=MESH,
            ).start()
        return carry

    lax.fori_loop(0, n_in, project, 0)

    def reduced(c):
        wait_bytes(precv.at[c, pl.ds(0, n_dp - 1)], p_recv.at[c])
        total = precv[c, 0].astype(F32)
        for p in range(1, n_dp):
            total = total + precv[c, p].astype(F32)
        return total

    def share(h, value):
        ag[h, i] = value
        for d in range(1, n_dp):
            p = lax.rem(i + d, n_dp)
            pltpu.make_async_remote_copy(
                src_ref=ag.at[h, i], dst_ref=ag.at[h, i],
                send_sem=g_send, recv_sem=g_recv.at[h],
                device_id=(p, j), device_id_type=MESH,
            ).start()

    query, key, value = reduced(0), reduced(1), reduced(2)
    mixed = []
    for h in range(wide // HEAD):
        cols = slice(h * HEAD, (h + 1) * HEAD)
        query_norm = normalize(query[:, cols].astype(BF16).astype(F32)).astype(BF16)
        key_norm = normalize(key[:, cols].astype(BF16).astype(F32)).astype(BF16)
        scores = lax.dot_general(
            query_norm, key_norm, (((1,), (1,)), ((), ())), preferred_element_type=F32
        )
        scores = scores * (temper[h] * (1.0 / math.sqrt(HEAD)))
        weight = jnp.exp(scores - jnp.max(scores, axis=-1, keepdims=True))
        probs = (weight / jnp.sum(weight, axis=-1, keepdims=True)).astype(BF16)
        mixed.append(
            jnp.dot(probs, value[:, cols].astype(BF16), preferred_element_type=F32).astype(BF16)
        )
    share(0, jnp.concatenate(mixed, axis=1))

    def activate(h, carry):
        at = pl.multiple_of((h - 1) * wide, HEAD)
        inner = reduced(h + 2) + bias[:, pl.ds(at, wide)]
        activ = 0.5 * inner * (1.0 + lax.erf(inner * math.sqrt(0.5)))
        share(h, activ.astype(BF16))
        return carry

    lax.fori_loop(1, n_out, activate, 0)

    acc[...] = jnp.zeros_like(acc)

    def project_out(h, carry):
        pltpu.make_async_copy(w_attn, w_out.at[h], wout_sem.at[h]).wait()
        wait_bytes(ag.at[h, pl.ds(0, n_dp - 1)], g_recv.at[h])
        acc[...] += jnp.dot(
            ag[h].reshape(n_dp * per, wide), w_out[h], preferred_element_type=F32
        ).reshape(acc.shape)
        return carry

    lax.fori_loop(0, n_out, project_out, 0)

    def halves(p, q):
        tile = acc[p, 2 * rows * q : 2 * rows * (q + 1), :]
        low, high = tile[:rows], tile[rows:]
        return jnp.where(core == 0, low, high), jnp.where(core == 0, high, low)

    for k in range(n_dp):
        p = lax.rem(i + 1 + k, n_dp)
        for q in range(n_chip):
            xsend[p, q] = halves(p, q)[1].astype(BF16)
        pltpu.make_async_remote_copy(
            src_ref=xsend.at[p], dst_ref=xrecv.at[p], send_sem=x_send, recv_sem=x_recv.at[k],
            device_id=sibling, device_id_type=MESH,
        ).start()

    for k in range(n_dp):
        p = lax.rem(i + 1 + k, n_dp)
        wait_bytes(xrecv.at[p], x_recv.at[k])
        for q in range(n_chip):
            dsend[p, q] = (halves(p, q)[0] + xrecv[p, q].astype(F32)).astype(BF16)

        def scatter_out(d, carry):
            q = lax.rem(chip + d, n_chip)
            pltpu.make_async_remote_copy(
                src_ref=dsend.at[p, q], dst_ref=drecv.at[lane], send_sem=d_send, recv_sem=d_recv,
                device_id=(p, 2 * q + core), device_id_type=MESH,
            ).start()
            return carry

        lax.fori_loop(1, n_chip if k == n_dp - 1 else n_chip + 1, scatter_out, 0)
    drecv[lane] = dsend[i, chip]
    wait_bytes(drecv.at[pl.ds(0, n_lane - 1)], d_recv)
    for p in range(n_dp):
        total = drecv[p * n_chip].astype(F32)
        for q in range(1, n_chip):
            total = total + drecv[p * n_chip + q].astype(F32)
        cols = slice(p * depth, (p + 1) * depth)
        out[:, cols] = (tokens[:, cols].astype(F32) + total).astype(BF16)

    wait_bytes(nrecv.at[pl.ds(0, n_lane - 1)], a_send)
    wait_bytes(nrecv.at[pl.ds(0, n_lane)], f_send)
    wait_bytes(precv.at[:, pl.ds(0, n_dp - 1)], p_send)
    wait_bytes(ag.at[:, pl.ds(0, n_dp - 1)], g_send)
    wait_bytes(xrecv, x_send)
    wait_bytes(drecv.at[pl.ds(0, n_lane - 1)], d_send)


def per_device(
    n_dp, n_mp,
    tokens, norm_gain, w_query, w_key, w_value, w_inner, bias_inner, w_attn_out, w_outer, temper
):
    rows, width = tokens.shape
    depth, wide = w_query.shape
    hidden = w_inner.shape[1]
    n_dev, per = n_dp * n_mp, n_mp * rows
    n_in, n_out = 3 + hidden // wide, 1 + hidden // wide
    vmem = pl.BlockSpec(memory_space=pltpu.VMEM)
    smem = pl.BlockSpec(memory_space=pltpu.SMEM)
    hbm = pl.BlockSpec(memory_space=pl.ANY)
    dma = pltpu.SemaphoreType.DMA
    return pl.pallas_call(
        functools.partial(block_kernel, n_dp, n_mp),
        out_shape=jax.ShapeDtypeStruct((rows, width), BF16),
        in_specs=[vmem, vmem, vmem, smem] + [hbm] * 6,
        out_specs=vmem,
        scratch_shapes=[
            pltpu.VMEM((n_in, depth, wide), BF16),
            pltpu.VMEM((n_out, wide, depth), BF16),
            pltpu.VMEM((n_dp, rows, depth), BF16),
            pltpu.VMEM((n_dev, rows, depth), BF16),
            pltpu.VMEM((n_dev * rows, depth), F32),
            pltpu.VMEM((n_dev * rows, depth), BF16),
            pltpu.VMEM((n_in, n_dp, per, wide), BF16),
            pltpu.VMEM((n_in, n_dp, per, wide), BF16),
            pltpu.VMEM((n_out, n_dp, per, wide), BF16),
            pltpu.VMEM((n_dp, per, depth), F32),
            pltpu.VMEM((n_dp, n_mp // 2, rows, depth), BF16),
            pltpu.VMEM((n_dp, n_mp // 2, rows, depth), BF16),
            pltpu.VMEM((n_dp, n_mp // 2, rows, depth), BF16),
            pltpu.VMEM((n_dev // 2, rows, depth), BF16),
            dma((n_in,)), dma((n_out,)), dma, dma((n_dev // 2,)), dma, dma, dma, dma((n_in,)),
            dma, dma((n_out,)), dma, dma((n_dp,)), dma, dma,
        ],
        compiler_params=pltpu.CompilerParams(
            collective_id=0, has_side_effects=True, vmem_limit_bytes=60 * 1024 * 1024
        ),
        name="encoder_block",
    )(
        tokens, norm_gain.reshape(1, -1), bias_inner.reshape(1, -1), temper,
        w_query, w_key, w_value, w_inner, w_attn_out, w_outer,
    )


def solution(mesh):
    return jax.shard_map(
        functools.partial(per_device, mesh.shape["dp"], mesh.shape["mp"]),
        mesh=mesh,
        in_specs=(
            P(("dp", "mp"), None),
            P(),
            P("dp", "mp"),
            P("dp", "mp"),
            P("dp", "mp"),
            P("dp", "mp"),
            P("mp"),
            P("mp", "dp"),
            P("mp", "dp"),
            P("mp"),
        ),
        out_specs=P(("dp", "mp"), None),
        check_vma=False,
    )
```

```python
import functools
import math

import jax
import jax.numpy as jnp
from jax import lax
from jax.experimental import pallas as pl
from jax.experimental.pallas import tpu as pltpu
from jax.sharding import PartitionSpec as P

HEAD = 128
LAG_SUM = 5
LAG_PASS = 7
MESH = pl.DeviceIdType.MESH
F32, BF16 = jnp.float32, jnp.bfloat16


def normalize(values):
    center = values - jnp.mean(values, axis=-1, keepdims=True)
    spread = jnp.mean(center * center, axis=-1, keepdims=True)
    return center * lax.rsqrt(spread + 1e-06)


def wait_bytes(ref, sem):
    pltpu.make_async_copy(ref, ref, sem).wait()


def block_kernel(
    n_dp, n_mp,
    tokens, gain, bias, temper, w_query, w_key, w_value, w_inner, w_attn, w_outer,
    out,
    w_in, w_out, nsend, nrecv, stage, x, psend, precv, ag, acc, xsend, xrecv, dsend, drecv,
    win_sem, wout_sem, a_send, a_recv, f_send, f_recv, p_send, p_recv, g_send, g_recv,
    x_send, x_recv, d_send, d_recv,
):
    n_dev = n_dp * n_mp
    rows = tokens.shape[0]
    n_in, depth, wide = w_in.shape
    n_out = w_out.shape[0]
    per = psend.shape[2]
    i, j = lax.axis_index("dp"), lax.axis_index("mp")
    me = i * n_mp + j
    n_chip = n_mp // 2
    n_lane = n_dp * n_chip
    core, chip = lax.rem(j, 2), j // 2
    sibling = (i, j + 1 - 2 * core)
    lane = i * n_chip + chip

    def same_core(other):
        return (other // n_chip, 2 * lax.rem(other, n_chip) + core)

    barrier = pltpu.get_barrier_semaphore()

    def greet(d, carry):
        t = lax.rem(me + d, n_dev)
        pl.semaphore_signal(
            barrier, inc=1, device_id=(t // n_mp, lax.rem(t, n_mp)), device_id_type=MESH
        )
        return carry

    lax.fori_loop(1, n_dev, greet, 0)

    for c, w in enumerate((w_query, w_key, w_value)):
        pltpu.make_async_copy(w, w_in.at[c], win_sem.at[c]).start()
    for c in range(3, n_in):
        pltpu.make_async_copy(
            w_inner.at[:, pl.ds((c - 3) * wide, wide)], w_in.at[c], win_sem.at[c]
        ).start()
    pltpu.make_async_copy(w_attn, w_out.at[0], wout_sem.at[0]).start()
    for c in range(1, n_out):
        pltpu.make_async_copy(
            w_outer.at[pl.ds((c - 1) * wide, wide), :], w_out.at[c], wout_sem.at[c]
        ).start()

    normed = (normalize(tokens[...].astype(F32)) * gain[...]).astype(BF16)
    for p in range(n_dp):
        nsend[p] = normed[:, p * depth : (p + 1) * depth]
    nrecv[me] = nsend[i]
    pl.semaphore_wait(barrier, n_dev - 1)

    def scatter_normed(d, carry):
        target = same_core(lax.rem(lane + d, n_lane))
        pltpu.make_async_remote_copy(
            src_ref=nsend.at[target[0]], dst_ref=nrecv.at[me],
            send_sem=a_send, recv_sem=a_recv.at[d],
            device_id=target, device_id_type=MESH,
        ).start()
        return carry

    def pass_on(source):
        pltpu.make_async_remote_copy(
            src_ref=nrecv.at[source], dst_ref=nrecv.at[source], send_sem=f_send, recv_sem=f_recv,
            device_id=sibling, device_id_type=MESH,
        ).start()

    lax.fori_loop(1, n_lane, scatter_normed, 0)
    pass_on(me)

    def forward_normed(d, carry):
        wait_bytes(nrecv.at[0], a_recv.at[d])
        source = same_core(lax.rem(lane + n_lane - d, n_lane))
        pass_on(source[0] * n_mp + source[1])
        return carry

    lax.fori_loop(1, n_lane, forward_normed, 0)
    wait_bytes(nrecv.at[pl.ds(0, n_lane)], f_recv)
    for s in range(n_dev):
        stage[s * rows : (s + 1) * rows, :] = nrecv[s].astype(F32)
    x[...] = stage[...].astype(BF16)

    square = n_dp == 4

    def around(c):
        beside = i + 1 - 2 * lax.rem(i, 2)
        across = lax.rem(i + 2, n_dp)
        turn = lax.rem(c, 2)
        return beside + turn * (across - beside), across + turn * (beside - across)

    def send(source, target, send_sem, recv_sem, p):
        pltpu.make_async_remote_copy(
            src_ref=source, dst_ref=target, send_sem=send_sem, recv_sem=recv_sem,
            device_id=(p, j), device_id_type=MESH,
        ).start()

    def project(c, carry):
        pltpu.make_async_copy(w_query, w_in.at[c], win_sem.at[c]).wait()
        part = jnp.dot(x[...], w_in[c], preferred_element_type=F32).astype(BF16)
        psend[c] = part.reshape(n_dp, per, wide)
        if square:
            first, _ = around(c)
            send(psend.at[c, 3 - i], precv.at[c, 1], p_send, p_recv.at[c, 1], first)
            send(psend.at[c, first], precv.at[c, 0], p_send, p_recv.at[c, 0], first)
            pl.when(c >= LAG_SUM)(lambda: add_and_send(c - LAG_SUM))
        else:
            precv[c, i] = psend[c, i]
            for d in range(1, n_dp):
                p = lax.rem(i + d, n_dp)
                send(psend.at[c, p], precv.at[c, i], p_send, p_recv.at[c, 0], p)
        return carry

    def add_and_send(c):
        _, second = around(c)
        wait_bytes(precv.at[c, 1], p_recv.at[c, 1])
        precv[c, 3] = (psend[c, second].astype(F32) + precv[c, 1].astype(F32)).astype(BF16)
        send(precv.at[c, 3], precv.at[c, 2], p_send, p_recv.at[c, 2], second)

    lax.fori_loop(0, n_in, project, 0)
    if square:
        for c in range(max(n_in - LAG_SUM, 0), n_in):
            add_and_send(c)

    def reduced(c):
        if square:
            wait_bytes(precv.at[c, 0], p_recv.at[c, 0])
            wait_bytes(precv.at[c, 2], p_recv.at[c, 2])
            total = psend[c, i].astype(F32) + precv[c, 0].astype(F32)
            return total + precv[c, 2].astype(F32)
        wait_bytes(precv.at[c, pl.ds(0, n_dp - 1)], p_recv.at[c, 0])
        total = precv[c, 0].astype(F32)
        for p in range(1, n_dp):
            total = total + precv[c, p].astype(F32)
        return total

    def share(h, value):
        ag[h, i] = value
        own = ag.at[h, i]
        if square:
            first, second = around(h)
            send(own, own, g_send, g_recv.at[h, 0], second)
            send(own, own, g_send, g_recv.at[h, 1], first)
        else:
            for d in range(1, n_dp):
                send(own, own, g_send, g_recv.at[h, 0], lax.rem(i + d, n_dp))

    def hand_over(h):
        first, second = around(h)
        block = ag.at[h, second]
        wait_bytes(block, g_recv.at[h, 0])
        send(block, block, g_send, g_recv.at[h, 2], first)

    query, key, value = reduced(0), reduced(1), reduced(2)
    mixed = []
    for h in range(wide // HEAD):
        cols = slice(h * HEAD, (h + 1) * HEAD)
        query_norm = normalize(query[:, cols].astype(BF16).astype(F32)).astype(BF16)
        key_norm = normalize(key[:, cols].astype(BF16).astype(F32)).astype(BF16)
        scores = lax.dot_general(
            query_norm, key_norm, (((1,), (1,)), ((), ())), preferred_element_type=F32
        )
        scores = scores * (temper[h] * (1.0 / math.sqrt(HEAD)))
        weight = jnp.exp(scores - jnp.max(scores, axis=-1, keepdims=True))
        probs = (weight / jnp.sum(weight, axis=-1, keepdims=True)).astype(BF16)
        mixed.append(
            jnp.dot(probs, value[:, cols].astype(BF16), preferred_element_type=F32).astype(BF16)
        )
    share(0, jnp.concatenate(mixed, axis=1))

    def activate(h, carry):
        at = pl.multiple_of((h - 1) * wide, HEAD)
        inner = reduced(h + 2) + bias[:, pl.ds(at, wide)]
        activ = 0.5 * inner * (1.0 + lax.erf(inner * math.sqrt(0.5)))
        share(h, activ.astype(BF16))
        if square:
            pl.when(h >= LAG_PASS)(lambda: hand_over(h - LAG_PASS))
        return carry

    lax.fori_loop(1, n_out, activate, 0)
    if square:
        for h in range(max(n_out - LAG_PASS, 0), n_out):
            hand_over(h)

    acc[...] = jnp.zeros_like(acc)

    def project_out(h, carry):
        pltpu.make_async_copy(w_attn, w_out.at[h], wout_sem.at[h]).wait()
        if square:
            wait_bytes(ag.at[h, 0], g_recv.at[h, 1])
            wait_bytes(ag.at[h, 0], g_recv.at[h, 2])
        else:
            wait_bytes(ag.at[h, pl.ds(0, n_dp - 1)], g_recv.at[h, 0])
        acc[...] += jnp.dot(
            ag[h].reshape(n_dp * per, wide), w_out[h], preferred_element_type=F32
        ).reshape(acc.shape)
        return carry

    lax.fori_loop(0, n_out, project_out, 0)

    def halves(p, q):
        tile = acc[p, 2 * rows * q : 2 * rows * (q + 1), :]
        low, high = tile[:rows], tile[rows:]
        return jnp.where(core == 0, low, high), jnp.where(core == 0, high, low)

    for k in range(n_dp):
        p = lax.rem(i + 1 + k, n_dp)
        for q in range(n_chip):
            xsend[p, q] = halves(p, q)[1].astype(BF16)
        pltpu.make_async_remote_copy(
            src_ref=xsend.at[p], dst_ref=xrecv.at[p], send_sem=x_send, recv_sem=x_recv.at[k],
            device_id=sibling, device_id_type=MESH,
        ).start()

    for k in range(n_dp):
        p = lax.rem(i + 1 + k, n_dp)
        wait_bytes(xrecv.at[p], x_recv.at[k])
        for q in range(n_chip):
            dsend[p, q] = (halves(p, q)[0] + xrecv[p, q].astype(F32)).astype(BF16)

        def scatter_out(d, carry):
            q = lax.rem(chip + d, n_chip)
            pltpu.make_async_remote_copy(
                src_ref=dsend.at[p, q], dst_ref=drecv.at[lane], send_sem=d_send, recv_sem=d_recv,
                device_id=(p, 2 * q + core), device_id_type=MESH,
            ).start()
            return carry

        lax.fori_loop(1, n_chip if k == n_dp - 1 else n_chip + 1, scatter_out, 0)
    drecv[lane] = dsend[i, chip]
    wait_bytes(drecv.at[pl.ds(0, n_lane - 1)], d_recv)
    for p in range(n_dp):
        total = drecv[p * n_chip].astype(F32)
        for q in range(1, n_chip):
            total = total + drecv[p * n_chip + q].astype(F32)
        cols = slice(p * depth, (p + 1) * depth)
        out[:, cols] = (tokens[:, cols].astype(F32) + total).astype(BF16)

    wait_bytes(nrecv.at[pl.ds(0, n_lane - 1)], a_send)
    wait_bytes(nrecv.at[pl.ds(0, n_lane)], f_send)
    wait_bytes(precv.at[:, pl.ds(0, n_dp - 1)], p_send)
    wait_bytes(ag.at[:, pl.ds(0, n_dp - 1)], g_send)
    wait_bytes(xrecv, x_send)
    wait_bytes(drecv.at[pl.ds(0, n_lane - 1)], d_send)


def per_device(
    n_dp, n_mp,
    tokens, norm_gain, w_query, w_key, w_value, w_inner, bias_inner, w_attn_out, w_outer, temper
):
    rows, width = tokens.shape
    depth, wide = w_query.shape
    hidden = w_inner.shape[1]
    n_dev, per = n_dp * n_mp, n_mp * rows
    n_in, n_out = 3 + hidden // wide, 1 + hidden // wide
    vmem = pl.BlockSpec(memory_space=pltpu.VMEM)
    smem = pl.BlockSpec(memory_space=pltpu.SMEM)
    hbm = pl.BlockSpec(memory_space=pl.ANY)
    dma = pltpu.SemaphoreType.DMA
    return pl.pallas_call(
        functools.partial(block_kernel, n_dp, n_mp),
        out_shape=jax.ShapeDtypeStruct((rows, width), BF16),
        in_specs=[vmem, vmem, vmem, smem] + [hbm] * 6,
        out_specs=vmem,
        scratch_shapes=[
            pltpu.VMEM((n_in, depth, wide), BF16),
            pltpu.VMEM((n_out, wide, depth), BF16),
            pltpu.VMEM((n_dp, rows, depth), BF16),
            pltpu.VMEM((n_dev, rows, depth), BF16),
            pltpu.VMEM((n_dev * rows, depth), F32),
            pltpu.VMEM((n_dev * rows, depth), BF16),
            pltpu.VMEM((n_in, n_dp, per, wide), BF16),
            pltpu.VMEM((n_in, n_dp, per, wide), BF16),
            pltpu.VMEM((n_out, n_dp, per, wide), BF16),
            pltpu.VMEM((n_dp, per, depth), F32),
            pltpu.VMEM((n_dp, n_mp // 2, rows, depth), BF16),
            pltpu.VMEM((n_dp, n_mp // 2, rows, depth), BF16),
            pltpu.VMEM((n_dp, n_mp // 2, rows, depth), BF16),
            pltpu.VMEM((n_dev // 2, rows, depth), BF16),
            dma((n_in,)), dma((n_out,)), dma, dma((n_dev // 2,)), dma, dma, dma, dma((n_in, 3)),
            dma, dma((n_out, 3)), dma, dma((n_dp,)), dma, dma,
        ],
        compiler_params=pltpu.CompilerParams(
            collective_id=0, has_side_effects=True, vmem_limit_bytes=60 * 1024 * 1024
        ),
        name="encoder_block",
    )(
        tokens, norm_gain.reshape(1, -1), bias_inner.reshape(1, -1), temper,
        w_query, w_key, w_value, w_inner, w_attn_out, w_outer,
    )


def solution(mesh):
    return jax.shard_map(
        functools.partial(per_device, mesh.shape["dp"], mesh.shape["mp"]),
        mesh=mesh,
        in_specs=(
            P(("dp", "mp"), None),
            P(),
            P("dp", "mp"),
            P("dp", "mp"),
            P("dp", "mp"),
            P("dp", "mp"),
            P("mp"),
            P("mp", "dp"),
            P("mp", "dp"),
            P("mp"),
        ),
        out_specs=P(("dp", "mp"), None),
        check_vma=False,
    )
```
